256 devices in a mesh: arcs: 16 (over x, y_hi, core), tiles: 16 (over z, y_lo).
Axes of the slice: x: 4, y: 4 (y_hi: 2, y_lo: 2; y = y_hi * 2 + y_lo), z: 8, core: 2. Of those that a mesh axis runs over, the one named last changes fastest.
Arguments:
- design: bfloat16 [24576, 8192], P('arcs', 'tiles'), may hold values from -0.09375 to 0.09375
- observations: float32 [24576], P('arcs'), may hold values from -25 to 25
- solution: float32 [8192], P('tiles'), may hold values from -6 to 6
- arc_ids: int32 [16, 1536], P('arcs'), may hold values from 0 to 3, never falling along the last dimension, each value on 1 to 768 neighbouring positions
- block_live: int32 [16, 12], P('arcs'), may hold values 0 or 1
Outputs:
- normal: float32 [8192, 8192], P('arcs', 'tiles')
- rhs: float32 [8192], P('tiles')
The draws below stay inside these ranges and needn't reach their ends.
Inputs may be any that keep to these rules, and one draw needn't show every extreme that they name: `arc_ids`: the arcs of a group's rows never fall along its rows; an arc holds at most 768 rows and some arc exactly that many.
All inputs are finite; a program needn't handle non-finite values. No bound on the sum of `block_live` on one device may be relied on, other than what follows from the above.
Results may differ from the reference program's by a relative error of at most 0.0018.
Values may be sent and summed in bfloat16 or wider, within the bound.
A program may use at most 128 MiB of HBM per device.

```python
import math
import jax
import jax.numpy as jnp
import numpy as np
from jax import lax

COEF = 8192
ROWS_DEV = 1536
ARCS_DEV = 4
SEG_MOST = 768
BLOCKS = 12
TOTAL_ROWS = 24576
N_ARCS = 16


def draw_observations(key, part):
    first_key, second_key = jax.random.split(jax.random.fold_in(key, 11))
    position = jnp.arange(TOTAL_ROWS, dtype=jnp.int32)
    denominator = max(TOTAL_ROWS // ROWS_DEV - 1, 1)
    device_frac = (position // ROWS_DEV).astype(jnp.float32) / denominator
    group_scale = jnp.exp(jax.random.uniform(second_key, (TOTAL_ROWS // 64,), minval=-0.5, maxval=0.5))
    local_scale = jnp.repeat(group_scale, 64)
    noise = jnp.clip(jax.random.normal(first_key, (TOTAL_ROWS,)), -5.0, 5.0)
    return (noise * (1.0 + 2.0 * device_frac) * local_scale).astype(jnp.float32)


def set_ends(result, stream_key, low, high):
    index_at = [jax.random.randint(jax.random.fold_in(stream_key, axis), (), 0, length) for axis, length in enumerate(result.shape)]
    longest = result.shape.index(max(result.shape))
    neighbour = index_at[:longest] + [(index_at[longest] + 1) % result.shape[longest]] + index_at[longest + 1:]
    return result.at[tuple(index_at)].set(low).at[tuple(neighbour)].set(high)


def raised(drawn, stream_key, source, target, parts, factor):
    owner, partner = [(jnp.arange(drawn.shape[dim]) // (drawn.shape[dim] // parts)).reshape([-1 if axis == dim else 1 for axis in range(drawn.ndim)]) for dim in (source, target)]
    chosen = jax.random.permutation(stream_key, parts)[partner]
    strong = (owner == chosen) | (owner == (partner + parts // 2) % parts)
    return jnp.where(strong, factor * drawn, drawn)


def shard_levels(own_key, dims, cuts, low, largest):
    def one(dim, blocks):
        steps = jax.random.uniform(jax.random.fold_in(jax.random.fold_in(own_key, 6), dim), (blocks,), jnp.float32, low / len(cuts), largest / len(cuts))
        return jnp.repeat(jnp.exp(steps), dims[dim] // blocks).reshape((-1,) + (1,) * (len(dims) - dim - 1))

    level = one(*cuts[0])
    for cut in cuts[1:]:
        level = level * one(*cut)
    return level


def split_up(number_of, total, bound, skew):
    portions = [(1 << 20) // math.isqrt(standing ** skew) + 1 for standing in range(2, number_of + 1)]
    spare, holding = total - bound - (number_of - 1), [1] * (number_of - 1)
    while spare > 0:
        free = [i for i in range(number_of - 1) if holding[i] < bound]
        whole, budget = sum([portions[i] for i in free]), spare
        for i in free:
            more = min(bound - holding[i], max(1, budget * portions[i] // whole), spare)
            holding[i] = holding[i] + more
            spare = spare - more
    return np.array([bound] + holding)


def uneven(own_key, amount, total, most, skew):
    if amount == 2:
        one = jax.random.randint(own_key, (), max(1, total - most), min(most, total - 1) + 1)
        return jnp.stack([one, total - one])
    tallies = jnp.asarray(split_up(amount, total, most, skew), jnp.int32)
    twos = (amount - 1) // 2
    giver, receiver = tallies[1:1 + 2 * twos:2], tallies[2:2 + 2 * twos:2]
    margin = jnp.minimum(giver - 1, most - receiver)
    moved = jax.random.randint(jax.random.fold_in(own_key, 1), (twos,), 0, 1 << 20) % (margin + 1)
    tallies = tallies.at[1:1 + 2 * twos:2].set(giver - moved).at[2:2 + 2 * twos:2].set(receiver + moved)
    return tallies[jax.random.permutation(jax.random.fold_in(own_key, 2), amount)]


def gaussian(rng, shape, width, reach, cuts=(), kind=jnp.bfloat16):
    values = jax.random.normal(rng, shape, jnp.float32) * width
    if len(cuts) > 0:
        values = shard_levels(rng, shape, cuts, -0.22, 0.18) * values
    return jnp.clip(values, min=-reach, max=reach).astype(kind)


def gaussian_with(own_key, shape, width, limit, pieces, heavy, kind=jnp.bfloat16):
    entries = width * jax.random.normal(own_key, shape, jnp.float32)
    if pieces:
        entries = entries * shard_levels(own_key, shape, pieces, -0.22, 0.18)
    return jnp.clip(raised(entries, jax.random.fold_in(own_key, 3), *heavy), -limit, limit).astype(kind)


def setup_inputs(seed: int = 0) -> dict:
    key_of = jax.random.split(jax.random.key(seed), 6)
    design = gaussian_with(key_of[0], (TOTAL_ROWS, COEF), COEF ** -0.5, 0.09375, ((0, 16), (1, 16)), (0, 1, 16, 2.0))
    observations = draw_observations(jax.random.fold_in(key_of[5], 71), 0)
    solution = gaussian(key_of[2], (COEF,), 1.0, 6.0, ((0, 16),), jnp.float32)
    arc_ids = jax.vmap(lambda own: jnp.searchsorted(jnp.cumsum(uneven(own, ARCS_DEV, ROWS_DEV, SEG_MOST, 2)), jnp.arange(ROWS_DEV), side="right"))(jax.random.split(key_of[3], N_ARCS)).reshape((N_ARCS, ROWS_DEV)).astype(jnp.int32)
    block_live = set_ends((jax.random.randint(key_of[4], (N_ARCS, BLOCKS), 0, 4) < 3).astype(jnp.int32), jax.random.fold_in(key_of[4], 1), 0, 1)
    return {"design": design, "observations": observations, "solution": solution, "arc_ids": arc_ids, "block_live": block_live}


prior_rows = 4.0


def reference(design, observations, solution, arc_ids, block_live):
    groups = arc_ids.shape[0]
    per_group = arc_ids.shape[1]
    row_count = groups * per_group
    live_row = jnp.broadcast_to(block_live[:, :, None], (groups, block_live.shape[1], 128)).reshape(row_count).astype(jnp.float32)
    design_wide = design.astype(jnp.float32)
    predicted = jnp.dot(design_wide, solution, precision=lax.Precision.HIGHEST)
    residual = observations - predicted
    squares = (live_row * residual * residual).reshape(groups, per_group)
    live_group = live_row.reshape(groups, per_group)
    arc_match = (arc_ids[:, None, :] == jnp.arange(ARCS_DEV, dtype=jnp.int32)[None, :, None]).astype(jnp.float32)
    arc_squares = jnp.sum(arc_match * squares[:, None, :], axis=2)
    arc_counts = jnp.sum(arc_match * live_group[:, None, :], axis=2)
    variance_all = (jnp.sum(arc_squares) + 1.0) / (jnp.sum(arc_counts) + 1.0)
    arc_weight = variance_all / ((arc_squares + prior_rows * variance_all) / (arc_counts + prior_rows))
    row_weight = live_row * jnp.sum(arc_match * arc_weight[:, :, None], axis=1).reshape(row_count)
    weighted = (row_weight[:, None] * design_wide).astype(jnp.bfloat16)
    normal = jnp.dot(design_wide.T, weighted.astype(jnp.float32), precision=lax.Precision.HIGHEST)
    rhs = jnp.dot(design_wide.T, row_weight * residual, precision=lax.Precision.HIGHEST)
    return normal, rhs
```

```python
import functools

import jax
import jax.numpy as jnp
from jax import lax
from jax.experimental import pallas as pl
from jax.experimental.pallas import tpu as pltpu
from jax.sharding import PartitionSpec as P

MESH = pl.DeviceIdType.MESH
F32 = jnp.float32
BF16 = jnp.bfloat16

ARCS_DEV = 4
PRIOR = 4.0
ROWS = 1536
COLS = 512
CHUNKS = 12
STEP = ROWS // CHUNKS
PEERS = 15
N = 10
LEAD = 6
EXACT = 3
PAIRS = (
    (0, 0, False),
    (3, 0, True),
    (3, 1, True),
    (3, 2, True),
    (4, 2, False),
    (2, 5, False),
    (1, 5, True),
    (0, 5, True),
    (3, 5, True),
    (4, 5, False),
)
SCALED = {0: 0, 1: 1, 2: 2, 5: 3}
LATE = (6, 7, 8, 5, 9)
MOVED = [
    sum(bool(PAIRS[p][0]) for p in batch) + sum(bool(PAIRS[p][1]) for p in batch if PAIRS[p][2])
    for batch in ((0, 1, 2, 3, 4), (6, 7, 8), (5, 9))
]


def parts_of(row, height):
    first = row.astype(BF16).astype(F32)
    rest = row - first
    second = rest.astype(BF16).astype(F32)
    third = (rest - second).astype(BF16).astype(F32)
    at = lax.broadcasted_iota(jnp.int32, (height, row.shape[1]), 0)
    zero = jnp.zeros((), F32)
    return jnp.where(
        at == 0, first, jnp.where(at == 1, second, jnp.where(at == 2, third, zero))
    ).astype(BF16)


def kernel(
    live_ref, design, obs_ref, sol_ref, ids_ref, out_ref, rhs_ref,
    below, below2, above, above2, across2, turned, plain, scaled, weight_row, weight_column,
    pred_all, sig_all, rhs_all, partial, from_core,
    one_out, one_in, two_out, two_in, two_own, three_out, three_in,
    spread_out, spread_in, own_piece, whole_all, moved,
    g_send, g_recv, small_send, small_recv, c_send, c_recv, one_send, one_recv,
    two_send, two_recv, three_send, three_recv, s_send, s_recv, m_send, m_recv, f_send, f_recv, l_sem,
):
    a = lax.axis_index("arcs")
    t = lax.axis_index("tiles")
    x, yh, c = a // 4, (a // 2) % 2, a % 2
    z, yl = t // 2, t % 2
    up = ((z + 1) % 8) * 2 + yl
    down = ((z + 7) % 8) * 2 + yl
    beside = z * 2 + (1 - yl)
    blocks = (design, below, below2, above, above2, across2)
    names = (
        t,
        down,
        ((z + 6) % 8) * 2 + yl,
        up,
        ((z + 2) % 8) * 2 + yl,
        ((z + 6) % 8) * 2 + (1 - yl),
    )
    near = x + 1 - 2 * (x % 2)
    far = 3 - x
    opposite = 3 - near

    barrier = pltpu.get_barrier_semaphore()
    for r in range(1, 16):
        pl.semaphore_signal(barrier, inc=1, device_id=(a, (t + r) % 16), device_id_type=MESH)
        pl.semaphore_signal(barrier, inc=1, device_id=((a + r) % 16, t), device_id_type=MESH)

    taps = parts_of(sol_ref[...], 16)
    for k in range(0, ROWS, 256):
        rows = slice(k, k + 256)
        value = lax.dot_general(
            taps, design[rows, :], (((1,), (1,)), ((), ())), preferred_element_type=F32
        )
        pred_all[t, :, rows] = jnp.sum(value, axis=0, keepdims=True)
    pl.semaphore_wait(barrier, 2 * PEERS)

    streams = (
        (design, below, up),
        (design, above, down),
        (below, below2, up),
        (above, above2, down),
        (below2, across2, beside),
    )

    def gather(s, k):
        src, dst, tile = streams[s]
        rows = pl.ds(k * STEP, STEP)
        return pltpu.make_async_remote_copy(
            src_ref=src.at[rows], dst_ref=dst.at[rows],
            send_sem=g_send.at[s], recv_sem=g_recv.at[s, k],
            device_id=(a, tile), device_id_type=MESH,
        )

    def small(buffer, me, which, device):
        return pltpu.make_async_remote_copy(
            src_ref=buffer.at[me], dst_ref=buffer.at[me],
            send_sem=small_send.at[which], recv_sem=small_recv.at[which],
            device_id=device, device_id_type=MESH,
        )

    def small_all(buffer, which):
        every = buffer.at[pl.ds(0, PEERS)]
        return pltpu.make_async_remote_copy(
            src_ref=every, dst_ref=every,
            send_sem=small_send.at[which], recv_sem=small_recv.at[which],
            device_id=(a, beside), device_id_type=MESH,
        )

    gather(0, 0).start()
    gather(1, 0).start()
    for r in range(1, 16):
        small(pred_all, t, 0, (a, (t + r) % 16)).start()
    for k in range(1, CHUNKS):
        if k < LEAD:
            gather(0, k).start()
        gather(1, k).start()

    def pass_up(k):
        gather(0, k).wait_recv()
        gather(2, k).start()
        if k + LEAD < CHUNKS:
            gather(0, k + LEAD).start()

    small_all(pred_all, 0).wait_recv()
    pass_up(0)
    pass_up(1)
    predicted = pred_all[0]
    for i in range(1, 16):
        predicted = predicted + pred_all[i]
    observed = jnp.concatenate([obs_ref[i : i + 1, :] for i in range(12)], axis=1)
    residual = observed - predicted
    live = jnp.concatenate(
        [jnp.full((1, 128), live_ref[0, i].astype(F32), F32) for i in range(12)], axis=1
    )
    squares = live * residual * residual
    ids = ids_ref[...]
    matches = [(ids == k).astype(F32) for k in range(ARCS_DEV)]
    arc_squares = [jnp.sum(m * squares, axis=1, keepdims=True) for m in matches]
    arc_counts = [jnp.sum(m * live, axis=1, keepdims=True) for m in matches]
    sig_all[a, :, 0:128] = jnp.broadcast_to(sum(arc_squares[1:], arc_squares[0]), (1, 128))
    sig_all[a, :, 128:256] = jnp.broadcast_to(sum(arc_counts[1:], arc_counts[0]), (1, 128))
    for r in range(1, 16):
        small(sig_all, a, 1, ((a + r) % 16, t)).start()
    small_all(sig_all, 1).wait_recv()
    pass_up(2)
    pass_up(3)
    totals = sig_all[0]
    for i in range(1, 16):
        totals = totals + sig_all[i]
    sigma = (totals[:, 0:1] + 1.0) / (totals[:, 128:129] + 1.0)
    row_weight = jnp.zeros((1, ROWS), F32)
    for m, s, n in zip(matches, arc_squares, arc_counts):
        row_weight = row_weight + m * (sigma / ((s + PRIOR * sigma) / (n + PRIOR)))
    row_weight = live * row_weight
    weight_row[...] = row_weight
    rhs_part = lax.dot_general(
        parts_of(row_weight * residual, 16), design[...],
        (((1,), (0,)), ((), ())), preferred_element_type=F32,
    )
    rhs_all[a] = jnp.sum(rhs_part, axis=0, keepdims=True)
    for r in range(1, 16):
        small(rhs_all, a, 2, ((a + r) % 16, t)).start()

    for i in range(0, ROWS, 128):
        tile = jnp.broadcast_to(row_weight[:, i : i + 128], (128, 128))
        weight_column[i : i + 128, :] = tile.T

    def turn(q, k):
        block = blocks[q]
        rows = slice(k * STEP, (k + 1) * STEP)
        tile = block[rows, :].T
        plain[q, :, rows] = tile
        turned[q, :, rows] = (tile.astype(F32) * weight_row[:, rows]).astype(BF16)

    def scale(v, k):
        block, n = blocks[v], SCALED[v]
        rows = slice(k * STEP, (k + 1) * STEP)
        for j in range(0, COLS, 128):
            tile = block[rows, j : j + 128].astype(F32) * weight_column[rows, :]
            scaled[n, rows, j : j + 128] = tile.astype(BF16)

    def product(p, lo, hi):
        q, v, _ = PAIRS[p]
        n, block = SCALED[v], blocks[v]
        for i in range(0, COLS, 256):
            cols = slice(i, i + 256)
            value = jnp.dot(turned[q, :, lo:hi], block[lo:hi, cols], preferred_element_type=F32)
            value = value + jnp.dot(
                plain[q, :, lo:hi], scaled[n, lo:hi, cols], preferred_element_type=F32
            )
            value = 0.5 * value
            for half in (0, 1):
                rows = slice(half * 256, half * 256 + 256)
                if lo:
                    partial[p, half, :, cols] += value[rows, :]
                else:
                    partial[p, half, :, cols] = value[rows, :]

    def core_copy(p):
        return pltpu.make_async_remote_copy(
            src_ref=partial.at[p, 1 - c], dst_ref=from_core.at[p],
            send_sem=c_send.at[0], recv_sem=c_recv.at[p],
            device_id=(x * 4 + yh * 2 + (1 - c), t), device_id_type=MESH,
        )

    def multiply(p, lo, hi):
        product(p, lo, hi)
        if hi == ROWS:
            core_copy(p).start()

    def at(i):
        return pl.ds(pl.multiple_of(i * 128, 128), 128)

    def both(p, half, strip):
        rows = slice(half * 128, half * 128 + 128)
        return partial[p, c, rows, at(strip)] + from_core[p, rows, at(strip)]

    def first_copy(p, half):
        pieces = pl.ds(2 * half, 2)
        return pltpu.make_async_remote_copy(
            src_ref=one_out.at[p, pieces], dst_ref=one_in.at[p, pieces],
            send_sem=one_send.at[0], recv_sem=one_recv.at[p, half],
            device_id=((far if half else near) * 4 + yh * 2 + c, t), device_id_type=MESH,
        )

    def second_copy(p, half):
        return pltpu.make_async_remote_copy(
            src_ref=two_out.at[p, half], dst_ref=two_in.at[p, half],
            send_sem=two_send.at[0], recv_sem=two_recv.at[p, half],
            device_id=((near if half else far) * 4 + yh * 2 + c, t), device_id_type=MESH,
        )

    def third_copy(p):
        return pltpu.make_async_remote_copy(
            src_ref=three_out.at[p], dst_ref=three_in.at[p],
            send_sem=three_send.at[0], recv_sem=three_recv.at[p],
            device_id=(x * 4 + (1 - yh) * 2 + c, t), device_id_type=MESH,
        )

    def first(p):
        core_copy(p).wait_recv()
        for half, neighbour in ((0, near), (1, far)):
            one_out[p, 2 * half] = both(p, half, neighbour)
            one_out[p, 2 * half + 1] = both(p, half, opposite)
            first_copy(p, half).start()

    def second(p):
        for half, neighbour in ((0, far), (1, near)):
            first_copy(p, half).wait_recv()
            two_out[p, half] = both(p, half, neighbour) + one_in[p, 2 * half + 1]
            second_copy(p, half).start()
            two_own[p, half] = both(p, half, x) + one_in[p, 2 * half]

    def third(p):
        for half in (0, 1):
            second_copy(p, half).wait_recv()
        three_out[p] = two_own[p, 1 - yh] + two_in[p, 1 - yh]
        third_copy(p).start()
        own_piece[p] = two_own[p, yh] + two_in[p, yh]

    place = x * 2 + yh

    def spread_copy(p, r):
        peer = (place + r) % 8
        return pltpu.make_async_remote_copy(
            src_ref=spread_out.at[p - EXACT, peer], dst_ref=spread_in.at[p - EXACT, r - 1],
            send_sem=s_send.at[0], recv_sem=s_recv.at[p - EXACT],
            device_id=((peer // 2) * 4 + (peer % 2) * 2 + c, t), device_id_type=MESH,
        )

    def spread(p):
        core_copy(p).wait_recv()
        for i in range(4):
            for j in (0, 1):
                rows, cols = slice(j * 128, j * 128 + 128), slice(i * 128, i * 128 + 128)
                total = partial[p, c, rows, cols] + from_core[p, rows, cols]
                spread_out[p - EXACT, i * 2 + j] = total.astype(BF16)
        for r in range(1, 8):
            spread_copy(p, r).start()
        own_piece[p] = partial[p, c, at(yh), at(x)] + from_core[p, at(yh), at(x)]

    row_at = pl.multiple_of(c * 256 + yh * 128, 128)
    col_at = pl.multiple_of(x * 128, 128)

    def all_of(ref, sem, send):
        copy = pltpu.make_async_remote_copy(
            src_ref=ref, dst_ref=ref, send_sem=sem, recv_sem=sem,
            device_id=(a, beside), device_id_type=MESH,
        )
        if send:
            copy.wait_send()
        else:
            copy.wait_recv()

    def outputs(p):
        q, v, mirrored = PAIRS[p]
        return [(p, q, -p % 5 and 8 - p % 5)] + ([(N + p, 2 if v == 5 else v, p % 5)] if mirrored else [])

    def batch(p):
        return 0 if p < 5 else 1 + (p in (5, 9))

    def tile_copy(n, column, group, dz, part):
        return pltpu.make_async_remote_copy(
            src_ref=whole_all.at[n], dst_ref=moved.at[group, dz],
            send_sem=m_send.at[0], recv_sem=m_recv.at[part],
            device_id=(a, names[column]), device_id_type=MESH,
        )

    def deliver(p):
        total = own_piece[p]
        if p < EXACT:
            third_copy(p).wait_recv()
            total = total + three_in[p]
        else:
            all_of(spread_in.at[p - EXACT], s_recv.at[p - EXACT], False)
            for r in range(7):
                total = total + spread_in[p - EXACT, r].astype(F32)
        for n, column, dz in outputs(p):
            value = total.T if n < N else total
            if column:
                whole_all[n] = value
                tile_copy(n, column, p // 5, dz, batch(p)).start()
            else:
                moved[p // 5, dz] = value

    def settle(part):
        group = min(part, 1)
        all_of(moved.at[group, pl.ds(0, MOVED[part])], m_recv.at[part], False)
        for r in range(8):
            row = (place + r) % 8
            dz = (row + 8 - z) % 8
            due = True if part == 0 else (dz % 4 == 0) == (part == 2)
            mirrored = jnp.logical_and(dz >= 1, dz <= 3)
            r0 = pl.multiple_of(jnp.where(mirrored, row_at, col_at), 128)
            c0 = pl.multiple_of(jnp.where(mirrored, col_at, row_at), 128)
            side = yl if group == 0 else jnp.where(mirrored, yl, 1 - yl)
            tile = t if group == 0 else jnp.where(mirrored, beside, t)
            source = moved.at[group, dz]
            target = out_ref.at[pl.ds(r0, 128), pl.ds(c0, 128)]

            def away():
                pltpu.make_async_remote_copy(
                    src_ref=source, dst_ref=target,
                    send_sem=f_send.at[0], recv_sem=f_recv.at[0],
                    device_id=(row * 2 + side, tile), device_id_type=MESH,
                ).start()

            if r:
                pl.when(due)(away)
            else:
                here = side == c
                if group:
                    here = jnp.logical_and(here, jnp.logical_not(mirrored))

                @pl.when(jnp.logical_and(due, here))
                def _():
                    keep = pltpu.make_async_copy(source, target, l_sem.at[0])
                    keep.start()
                    keep.wait()

                pl.when(jnp.logical_and(due, jnp.logical_not(here)))(away)

    def rhs_total():
        small_all(rhs_all, 2).wait_recv()
        rhs = rhs_all[0]
        for i in range(1, 16):
            rhs = rhs + rhs_all[i]
        for i in range(4):
            rhs_ref[i : i + 1, :] = rhs[:, i * 128 : i * 128 + 128]

    def arrive(s, k):
        gather(s, k).wait_recv()

    plan = []

    def add(when, task, *args):
        plan.append((when, len(plan), task, args))

    unit, start = 2.97, 8.0
    order = [("own", k) for k in range(LEAD)]
    for k in range(CHUNKS):
        order.append(("on", k))
        if k + LEAD < CHUNKS:
            order.append(("own", k + LEAD))
    landed = {item: start + unit * (i + 1) for i, item in enumerate(order)}
    weights = 26.0
    for k in range(CHUNKS):
        own, on = landed["own", k], landed["on", k]
        straight = start + unit * (k + 1)
        straight_on = straight + unit * CHUNKS
        if k > 3:
            add(own, pass_up, k)
        add(straight, arrive, 1, k)
        add(straight, lambda k: gather(3, k).start(), k)
        add(on, arrive, 2, k)
        add(on, lambda k: gather(4, k).start(), k)
        add(straight_on, arrive, 3, k)
        add(on + unit + 2.0, arrive, 4, k)
        add(weights, turn, 0, k)
        add(weights, scale, 0, k)
        add(max(weights, own) + 0.2, turn, 1, k)
        add(max(weights, own) + 0.2, scale, 1, k)
        add(max(weights, straight) + 0.2, turn, 3, k)
        add(max(weights, on) + 0.2, turn, 2, k)
        add(max(weights, on) + 0.2, scale, 2, k)
        add(straight_on + 0.2, turn, 4, k)
        add(on + unit + 2.2, scale, 5, k)

    def last(kind, k):
        return landed[kind, k]

    end = landed["on", CHUNKS - 1]
    add(weights + 1, multiply, 0, 0, ROWS)
    add(start + unit * CHUNKS + 0.5, multiply, 1, 0, ROWS)
    add(last("own", CHUNKS - 1) + 0.5, multiply, 2, 0, ROWS)
    for p in (3, 4):
        add(last("on", 8) + 0.5 + p / 10, multiply, p, 0, 1152)
        add(end + 0.3 + p / 10, multiply, p, 1152, ROWS)
    late = end + unit + 2.2
    for p in range(5, N):
        add(last("on", 5) + unit + 2.5 + p / 2, multiply, p, 0, 768)
        add(last("on", 9) + unit + 2.5 + p / 10, multiply, p, 768, 1280)
        add(late + LATE.index(p) / 100, multiply, p, 1280, ROWS)
    ready = (weights + 3, start + unit * CHUNKS + 2, last("own", 11) + 2)
    for p in range(EXACT):
        for i, stage in enumerate((first, second, third, deliver)):
            add(ready[p] + 2 + 6 * i, stage, p)
    for p in (3, 4):
        add(end + 2 + 0.4 * (p - 3), spread, p)
        add(end + 11.2 + 0.4 * (p - 3), deliver, p)
    for i, p in enumerate(LATE):
        add(late + 1.6 + 0.9 * i, spread, p)
        add(end + 13.5 + 2.8 * i, deliver, p)
    add(end + 13.6 + 2.8 * 2, settle, 0)
    add(end + 50, settle, 1)
    add(end + 51, settle, 2)
    add(end + 1, rhs_total)
    for _, _, task, args in sorted(plan, key=lambda item: item[:2]):
        task(*args)

    for s in range(5):
        all_of(design, g_send.at[s], True)
    small_all(pred_all, 0).wait_send()
    small_all(sig_all, 1).wait_send()
    small_all(rhs_all, 2).wait_send()
    all_of(from_core, c_send.at[0], True)
    all_of(one_out, one_send.at[0], True)
    all_of(two_out, two_send.at[0], True)
    all_of(spread_in, s_send.at[0], True)
    all_of(three_out, three_send.at[0], True)
    all_of(whole_all.at[pl.ds(0, sum(MOVED))], m_send.at[0], True)
    gap = (place + 8 - z) % 8
    crossed = jnp.logical_and(c != yl, jnp.logical_and(gap >= 1, gap <= 3))

    def settled(count):
        every = whole_all.at[pl.ds(0, count)]
        all_of(every, f_send.at[0], True)
        all_of(every, f_recv.at[0], False)

    pl.when(crossed)(lambda: settled(16))
    pl.when(jnp.logical_not(crossed))(lambda: settled(15))


def local(design, observations, solution, arc_ids, block_live):
    vmem = pl.BlockSpec(memory_space=pltpu.VMEM)
    normal, rhs = pl.pallas_call(
        kernel,
        out_shape=(
            jax.ShapeDtypeStruct((COLS, COLS), F32),
            jax.ShapeDtypeStruct((4, 128), F32),
        ),
        in_specs=[pl.BlockSpec(memory_space=pltpu.SMEM)] + [vmem] * 4,
        out_specs=(pl.BlockSpec(memory_space=pltpu.HBM), vmem),
        scratch_shapes=[pltpu.VMEM((ROWS, COLS), BF16)] * 5
        + [
            pltpu.VMEM((5, COLS, ROWS), BF16),
            pltpu.VMEM((5, COLS, ROWS), BF16),
            pltpu.VMEM((4, ROWS, COLS), BF16),
            pltpu.VMEM((1, ROWS), F32),
            pltpu.VMEM((ROWS, 128), F32),
            pltpu.VMEM((16, 1, ROWS), F32),
            pltpu.VMEM((16, 1, 256), F32),
            pltpu.VMEM((16, 1, COLS), F32),
        ]
        + [pltpu.VMEM((N, 2, 256, COLS), F32), pltpu.VMEM((N, 256, COLS), F32)]
        + [pltpu.VMEM((EXACT, 4, 128, 128), F32)] * 2
        + [pltpu.VMEM((EXACT, 2, 128, 128), F32)] * 3
        + [pltpu.VMEM((EXACT, 128, 128), F32)] * 2
        + [
            pltpu.VMEM((N - EXACT, 8, 128, 128), BF16),
            pltpu.VMEM((N - EXACT, 7, 128, 128), BF16),
            pltpu.VMEM((N, 128, 128), F32),
        ]
        + [pltpu.VMEM((2 * N, 128, 128), F32), pltpu.VMEM((2, 8, 128, 128), F32)]
        + [
            pltpu.SemaphoreType.DMA((5,)),
            pltpu.SemaphoreType.DMA((5, CHUNKS)),
            pltpu.SemaphoreType.DMA((3,)),
            pltpu.SemaphoreType.DMA((3,)),
            pltpu.SemaphoreType.DMA((1,)),
            pltpu.SemaphoreType.DMA((N,)),
            pltpu.SemaphoreType.DMA((1,)),
            pltpu.SemaphoreType.DMA((EXACT, 2)),
            pltpu.SemaphoreType.DMA((1,)),
            pltpu.SemaphoreType.DMA((EXACT, 2)),
            pltpu.SemaphoreType.DMA((1,)),
            pltpu.SemaphoreType.DMA((EXACT,)),
            pltpu.SemaphoreType.DMA((1,)),
            pltpu.SemaphoreType.DMA((N - EXACT,)),
            pltpu.SemaphoreType.DMA((1,)),
            pltpu.SemaphoreType.DMA((3,)),
            pltpu.SemaphoreType.DMA((1,)),
            pltpu.SemaphoreType.DMA((1,)),
            pltpu.SemaphoreType.DMA((1,)),
        ],
        compiler_params=pltpu.CompilerParams(
            collective_id=0, has_side_effects=True, vmem_limit_bytes=60 * 1024 * 1024
        ),
        name="normal_equations",
    )(
        block_live,
        design,
        observations.reshape(12, 128),
        solution.reshape(1, COLS),
        arc_ids,
    )
    return normal, rhs.reshape(COLS)


def solution(mesh):
    return jax.shard_map(
        local,
        mesh=mesh,
        in_specs=(P("arcs", "tiles"), P("arcs"), P("tiles"), P("arcs", None), P("arcs", None)),
        out_specs=(P("arcs", "tiles"), P("tiles")),
        check_vma=False,
    )
```
